32 devices in a mesh: tm: 8 (over y, x, core), batch: 4 (over z).
Axes of the slice: x: 2, y: 2, z: 4, core: 2. Of those that a mesh axis runs over, the one named last changes fastest.
Arguments:
- obs_feats: bfloat16 [16, 512, 2048], P('batch', 'tm'), may hold values from -6 to 6
- next_feats: bfloat16 [16, 512, 2048], P('batch', 'tm'), may hold values from -6 to 6
- online_w: float32 [2048, 2048], P(('tm', 'batch')), may hold values from -6 to 6
- target_w: float32 [2048, 2048], P(('tm', 'batch')), may hold values from -6 to 6
- log_decay: float32 [2048], replicated, may hold values from -1 to 0, as said below
- step_scale: float32 [16, 512], P('batch', 'tm'), may hold values from 0.5 to 2
- online_heads: float32 [2, 2048], replicated, may hold values from -6 to 6
- target_heads: float32 [2, 2048], replicated, may hold values from -6 to 6
- reward: float32 [16, 512], P('batch', 'tm'), may hold values from -6 to 6
- next_action_log_prob: float32 [16, 512], P('batch', 'tm'), may hold values from -3 to 1
- resets: int32 [16, 512], P('batch', 'tm'), may hold values 0 or 1
- horizon: int32 [16], P('batch'), may hold values from 1 to 8
- burn_in: int32 [16], P('batch'), may hold values from 0 to 64
Outputs:
- grad_w: float32 [2048, 2048], P(('tm', 'batch'))
- new_target: float32 [2048, 2048], P(('tm', 'batch'))
- returns: float32 [16, 512], P('batch', 'tm')
The draws below stay inside these ranges and needn't reach their ends.
Inputs may be any that keep to these rules, and one draw needn't show every extreme that they name: `log_decay`: every entry is negative.
All inputs are finite; a program needn't handle non-finite values. No bound on the sum of `resets` on one device may be relied on, other than what follows from the above.
Results may differ from the reference program's by a relative error of at most 0.0059.
Values may be sent and summed in bfloat16 or wider, within the bound.
A program may use at most 128 MiB of HBM per device.

```python
import math
import jax
import jax.numpy as jnp
from jax import lax

D = 2048
H = 2048
T_DEV = 64
NMAX = 8
BURN_MAX = 64
B = 16
L = 512


def draw_log_decay(key, part):
    first, second, third = jax.random.split(key, 3)
    keep_share = 0.5
    fast_rate = jax.random.uniform(third, (H,), minval=0.67, maxval=0.96) / T_DEV
    slow = jax.random.uniform(first, (H,)) < keep_share
    slow_rate = jnp.log(10.0) / (2.0 * L) * jax.random.uniform(second, (H,), minval=0.05, maxval=1.0)
    return (-jnp.where(slow, slow_rate, fast_rate)).astype(jnp.float32)


def touch_ends(result, stream_key, smallest, high):
    shape = result.shape
    place = [jax.random.randint(jax.random.fold_in(stream_key, axis), (), 0, shape[axis]) for axis in range(len(shape))]
    result = result.at[tuple(place)].set(smallest)
    longest = shape.index(max(shape))
    place[longest] = (place[longest] + 1) % shape[longest]
    return result.at[tuple(place)].set(high)


def with_spikes(result, stream_key, source, target, shards_of, factor):
    owner, partner = [(jnp.arange(result.shape[dim]) // (result.shape[dim] // shards_of)).reshape([-1 if axis == dim else 1 for axis in range(result.ndim)]) for dim in (source, target)]
    chosen = jax.random.permutation(stream_key, shards_of)[partner]
    strong = (owner == chosen) | (owner == (partner + shards_of // 2) % shards_of)
    return jnp.where(strong, factor * result, result)


def levels(rng, dims, cuts, smallest, largest):
    gain, own = 1.0, jax.random.fold_in(rng, 6)
    for position, shards_of in cuts:
        heights = jnp.exp(jax.random.uniform(jax.random.fold_in(own, position), (shards_of,), jnp.float32, smallest / len(cuts), largest / len(cuts)))
        gain = gain * jnp.repeat(heights, dims[position] // shards_of).reshape([-1 if axis == position else 1 for axis in range(len(dims))])
    return gain


def scatter_about(stream_key, extent, width, most, cuts=(), kind=jnp.bfloat16):
    result = jax.random.normal(stream_key, extent, jnp.float32) * width
    if len(cuts) > 0:
        result = levels(stream_key, extent, cuts, -0.22, 0.18) * result
    return jnp.clip(result, min=-most, max=most).astype(kind)


def heavy_noise(stream_key, extent, deviation, most, shards, heavy, dtype=jnp.bfloat16):
    values = deviation * jax.random.normal(stream_key, extent, jnp.float32)
    if shards:
        values = values * levels(stream_key, extent, shards, -0.22, 0.18)
    return jnp.clip(with_spikes(values, jax.random.fold_in(stream_key, 3), *heavy), -most, most).astype(dtype)


def setup_inputs(seed: int = 0) -> dict:
    keys = jax.random.split(jax.random.key(seed), 14)
    obs_feats = heavy_noise(keys[0], (B, L, D), 1.0, 6.0, ((0, 4), (1, 8)), (0, 2, 4, 2.0))
    next_feats = scatter_about(keys[1], (B, L, D), 1.0, 6.0, ((0, 4), (1, 8)))
    online_w = scatter_about(keys[2], (D, H), 1.0, 6.0, ((0, 32),), jnp.float32)
    target_w = scatter_about(keys[3], (D, H), 1.0, 6.0, ((0, 32),), jnp.float32)
    log_decay = draw_log_decay(jax.random.fold_in(keys[13], 71), 0)
    step_scale = jnp.clip(jnp.exp(math.log(2.0) - 1.3862944 * jax.random.uniform(keys[5], (B, L), jnp.float32) ** levels(keys[5], (B, L), ((0, 4), (1, 8)), -0.2, 0.2)), 0.5, 2.0)
    online_heads = scatter_about(keys[6], (2, H), 1.0, 6.0, (), jnp.float32)
    target_heads = scatter_about(keys[7], (2, H), 1.0, 6.0, (), jnp.float32)
    reward = scatter_about(keys[8], (B, L), 1.0, 6.0, ((0, 4), (1, 8)), jnp.float32)
    next_action_log_prob = jnp.clip(-3.0 + 4.0 * jax.random.uniform(keys[9], (B, L), jnp.float32) ** levels(keys[9], (B, L), ((0, 4), (1, 8)), -0.2, 0.2), -3.0, 1.0)
    resets = touch_ends((jax.random.randint(keys[10], (B, L), 0, 256) < 1).astype(jnp.int32), jax.random.fold_in(keys[10], 1), 0, 1)
    horizon = touch_ends(jax.random.randint(keys[11], (B,), 1, NMAX + 1), jax.random.fold_in(keys[11], 1), 1, NMAX).astype(jnp.int32)
    burn_in = touch_ends(jax.random.randint(keys[12], (B,), 0, BURN_MAX + 1), jax.random.fold_in(keys[12], 1), 0, BURN_MAX).astype(jnp.int32)
    return {"obs_feats": obs_feats, "next_feats": next_feats, "online_w": online_w, "target_w": target_w, "log_decay": log_decay, "step_scale": step_scale, "online_heads": online_heads, "target_heads": target_heads, "reward": reward, "next_action_log_prob": next_action_log_prob, "resets": resets, "horizon": horizon, "burn_in": burn_in}


DISCOUNT = 0.99
ENTROPY_COEFF = 0.2
POLYAK_RATE = 0.005
STEP_SIZE = 0.1

def affine(earlier, later):
    return (later[0] * earlier[0], later[0] * earlier[1] + later[1])

def silu_slope(values):
    sigma = jax.nn.sigmoid(values)
    return sigma * (1.0 + values * (1.0 - sigma))

def returns_from(ext_reward, ext_value, ext_keep, row_horizon, span):
    total = jnp.zeros((ext_reward.shape[0], span), jnp.float32)
    alive = jnp.ones((ext_reward.shape[0], span), jnp.float32)
    for offset in range(NMAX):
        inside = (row_horizon > offset)[:, None]
        total = total + jnp.where(inside, DISCOUNT ** offset * alive * ext_reward[:, offset:offset + span], 0.0)
        alive = alive * ext_keep[:, offset + 1:offset + 1 + span]
        finish = (row_horizon == offset + 1)[:, None]
        total = total + jnp.where(finish, DISCOUNT ** (offset + 1) * alive * ext_value[:, offset + 1:offset + 1 + span], 0.0)
    return total

def reference(obs_feats, next_feats, online_w, target_w, log_decay, step_scale, online_heads, target_heads, reward, next_action_log_prob, resets, horizon, burn_in):
    w_online = online_w.astype(jnp.bfloat16)
    w_target = target_w.astype(jnp.bfloat16)
    input_scale = D ** (-0.5)
    scale_head = H ** (-0.5)
    padding = jnp.zeros((NMAX,), jnp.float32)
    times = jnp.arange(L).astype(jnp.int32)

    def per_row(total_grad, row):
        inputs, inputs_next, stride, gains, action_log_prob, flags, row_horizon, row_burn = row
        decay = jnp.exp(stride[:, None] * log_decay[None, :])
        keeping = 1.0 - flags.astype(jnp.float32)
        factor = decay * keeping[:, None]
        spread = jnp.sqrt(1.0 - decay * decay)
        proj_on = jnp.dot(inputs, w_online, preferred_element_type=jnp.float32) * input_scale
        proj_tg = jnp.dot(inputs_next, w_target, preferred_element_type=jnp.float32) * input_scale
        state_on = lax.associative_scan(affine, (factor, spread * proj_on), axis=0)[1]
        state_tg = lax.associative_scan(affine, (factor, spread * proj_tg), axis=0)[1]
        q_on = jnp.dot(jax.nn.silu(state_on), online_heads.T, precision=lax.Precision.HIGHEST) * scale_head
        target_quality = jnp.dot(jax.nn.silu(state_tg), target_heads.T, precision=lax.Precision.HIGHEST) * scale_head
        soft_value = lax.optimization_barrier(jnp.min(target_quality, axis=1)) - ENTROPY_COEFF * action_log_prob
        row_returns = returns_from(jnp.concatenate([gains, padding])[None], jnp.concatenate([soft_value, padding])[None], jnp.concatenate([keeping, padding])[None], row_horizon[None], L)[0]
        weight_mask = (times >= row_burn).astype(jnp.float32)
        slope = weight_mask[:, None] * (q_on - row_returns[:, None])
        grad_y = jnp.dot(slope, online_heads, precision=lax.Precision.HIGHEST) * scale_head
        grad_h = grad_y * silu_slope(state_on)
        shifted = jnp.concatenate([factor[1:], jnp.ones((1, H), jnp.float32)], axis=0)
        adjoint = lax.associative_scan(affine, (shifted, grad_h), reverse=True, axis=0)[1]
        grad_u = (spread * adjoint).astype(jnp.bfloat16)
        term = lax.dot_general(inputs, grad_u, (((0,), (0,)), ((), ())), preferred_element_type=jnp.float32) * input_scale
        return (total_grad + term, row_returns)
    grad_w, returns = lax.scan(per_row, jnp.zeros((D, H), jnp.float32), (obs_feats, next_feats, step_scale, reward, next_action_log_prob, resets, horizon, burn_in))
    new_target = (1.0 - POLYAK_RATE) * target_w + POLYAK_RATE * (online_w - STEP_SIZE * grad_w)
    return (grad_w, new_target, returns)
```

```python
import functools

import jax
import jax.numpy as jnp
from jax import lax
from jax.experimental import pallas as pl
from jax.experimental.pallas import tpu as pltpu
from jax.sharding import PartitionSpec as P

NMAX = 8
SUB = 8
HEADS = 2

DISCOUNT = 0.99
ENTROPY_COEFF = 0.2
POLYAK_RATE = 0.005
STEP_SIZE = 0.1


def returns_from(ext_reward, ext_value, ext_keep, row_horizon, span):
    total = jnp.zeros((ext_reward.shape[0], span), jnp.float32)
    alive = jnp.ones((ext_reward.shape[0], span), jnp.float32)
    for offset in range(NMAX):
        inside = (row_horizon > offset)[:, None]
        total = total + jnp.where(
            inside, DISCOUNT**offset * alive * ext_reward[:, offset : offset + span], 0.0
        )
        alive = alive * ext_keep[:, offset + 1 : offset + 1 + span]
        finish = (row_horizon == offset + 1)[:, None]
        total = total + jnp.where(
            finish,
            DISCOUNT ** (offset + 1) * alive * ext_value[:, offset + 1 : offset + 1 + span],
            0.0,
        )
    return total


def tile_scan(gain, value, place, reverse):
    for shift in (1, 2, 4):
        if reverse:
            inside, move = place < SUB - shift, SUB - shift
        else:
            inside, move = place >= shift, shift
        other_gain = jnp.where(inside, pltpu.roll(gain, move, 1), 1.0)
        other_value = jnp.where(inside, pltpu.roll(value, move, 1), 0.0)
        value = value + gain * other_value
        gain = gain * other_gain
    return gain, value


def forward_kernel(
    input_scale, x_ref, w_ref, factor_ref, spread_ref, heads_ref, q_ref, state_ref, carry_ref
):
    rows_b, block, width = x_ref.shape
    hid = w_ref.shape[1]

    @pl.when(pl.program_id(0) == 0)
    def _():
        carry_ref[...] = jnp.zeros_like(carry_ref)

    proj = jnp.dot(
        x_ref[...].reshape(rows_b * block, width), w_ref[...], preferred_element_type=jnp.float32
    )
    drive = (proj * input_scale).reshape(rows_b, block, hid) * spread_ref[...]
    place = lax.broadcasted_iota(jnp.int32, (rows_b, SUB, hid), 1)
    carry = carry_ref[...]
    for tile in range(block // SUB):
        at = slice(tile * SUB, (tile + 1) * SUB)
        gain, value = tile_scan(factor_ref[:, at, :], drive[:, at, :], place, False)
        state = value + gain * carry
        state_ref[:, at, :] = state
        carry = jnp.broadcast_to(state[:, SUB - 1 : SUB, :], state.shape)
    carry_ref[...] = carry
    state = state_ref[...].reshape(rows_b * block, hid)
    act = state / (1.0 + jnp.exp(-state))
    q_ref[0] = lax.dot_general(
        heads_ref[...],
        act,
        (((1,), (1,)), ((), ())),
        precision=lax.Precision.HIGHEST,
        preferred_element_type=jnp.float32,
    )


def backward_kernel(state_ref, after_ref, spread_ref, dq_ref, heads_ref, du_ref, carry_ref):
    rows_b, block, hid = state_ref.shape

    @pl.when(pl.program_id(0) == 0)
    def _():
        carry_ref[...] = jnp.zeros_like(carry_ref)

    grad_y = lax.dot_general(
        dq_ref[0],
        heads_ref[...],
        (((0,), (0,)), ((), ())),
        precision=lax.Precision.HIGHEST,
        preferred_element_type=jnp.float32,
    ).reshape(rows_b, block, hid)
    state = state_ref[...]
    sigma = 1.0 / (1.0 + jnp.exp(-state))
    grad_h = grad_y * (sigma * (1.0 + state * (1.0 - sigma)))
    place = lax.broadcasted_iota(jnp.int32, (rows_b, SUB, hid), 1)
    carry = carry_ref[...]
    pieces = [None] * (block // SUB)
    for tile in reversed(range(block // SUB)):
        at = slice(tile * SUB, (tile + 1) * SUB)
        gain, value = tile_scan(after_ref[:, at, :], grad_h[:, at, :], place, True)
        adjoint = value + gain * carry
        pieces[tile] = spread_ref[:, at, :] * adjoint
        carry = jnp.broadcast_to(adjoint[:, 0:1, :], adjoint.shape)
    carry_ref[...] = carry
    du_ref[...] = jnp.concatenate(pieces, axis=1).astype(jnp.bfloat16)


def forward(x, w, factor, spread, heads, block):
    rows_b, length, width = x.shape
    hid = w.shape[1]
    count = length // block
    whole = lambda j: (0, 0)
    part = lambda j: (0, j, 0)
    return pl.pallas_call(
        functools.partial(forward_kernel, width ** (-0.5)),
        grid=(count,),
        in_specs=[
            pl.BlockSpec((rows_b, block, width), part),
            pl.BlockSpec((width, hid), whole),
            pl.BlockSpec((rows_b, block, hid), part),
            pl.BlockSpec((rows_b, block, hid), part),
            pl.BlockSpec(heads.shape, whole),
        ],
        out_specs=[
            pl.BlockSpec((1, heads.shape[0], rows_b * block), lambda j: (j, 0, 0)),
            pl.BlockSpec((rows_b, block, hid), part),
        ],
        out_shape=[
            jax.ShapeDtypeStruct((count, heads.shape[0], rows_b * block), jnp.float32),
            jax.ShapeDtypeStruct((rows_b, length, hid), jnp.float32),
        ],
        scratch_shapes=[pltpu.VMEM((rows_b, SUB, hid), jnp.float32)],
        compiler_params=pltpu.CompilerParams(dimension_semantics=("arbitrary",)),
        cost_estimate=pl.CostEstimate(
            flops=2 * rows_b * length * width * hid,
            bytes_accessed=x.size * 2 + w.size * 2 + 3 * factor.size * 4,
            transcendentals=2 * factor.size,
        ),
    )(x, w, factor, spread, heads)


def backward(state, after, spread, dq, heads, block):
    rows_b, length, hid = state.shape
    count = length // block
    part = lambda j: (0, count - 1 - j, 0)
    return pl.pallas_call(
        backward_kernel,
        grid=(count,),
        in_specs=[
            pl.BlockSpec((rows_b, block, hid), part),
            pl.BlockSpec((rows_b, block, hid), part),
            pl.BlockSpec((rows_b, block, hid), part),
            pl.BlockSpec((1, heads.shape[0], rows_b * block), lambda j: (count - 1 - j, 0, 0)),
            pl.BlockSpec(heads.shape, lambda j: (0, 0)),
        ],
        out_specs=pl.BlockSpec((rows_b, block, hid), part),
        out_shape=jax.ShapeDtypeStruct((rows_b, length, hid), jnp.bfloat16),
        scratch_shapes=[pltpu.VMEM((rows_b, SUB, hid), jnp.float32)],
        compiler_params=pltpu.CompilerParams(dimension_semantics=("arbitrary",)),
        cost_estimate=pl.CostEstimate(
            flops=40 * state.size,
            bytes_accessed=3 * state.size * 4 + state.size * 2,
            transcendentals=2 * state.size,
        ),
    )(state, after, spread, dq, heads)


def shards(
    obs_feats,
    next_feats,
    online_w,
    target_w,
    log_decay,
    step_scale,
    online_heads,
    target_heads,
    reward,
    next_action_log_prob,
    resets,
    horizon,
    burn_in,
):
    rows_b, span, width = obs_feats.shape
    hidden = online_w.shape[1]
    n_tm, n_b = lax.axis_size("tm"), lax.axis_size("batch")
    length = span * n_tm
    hid = hidden // n_tm
    mine = lax.axis_index("tm")
    both = ("tm", "batch")
    block = span
    count = length // block
    scale_head = hidden ** (-0.5)
    local_rows = online_w.shape[0]

    small = jnp.stack([step_scale, 1.0 - resets.astype(jnp.float32), reward, next_action_log_prob])
    small = lax.all_gather(small, "tm", axis=2, tiled=True)
    weights = jnp.stack([online_w, target_w]).astype(jnp.bfloat16)
    weights = weights.reshape(2, local_rows, n_tm, hid).transpose(2, 0, 1, 3)
    weights = jnp.broadcast_to(
        weights[:, None], (n_tm, n_b, 2, local_rows, hid)
    ).reshape(n_tm * n_b, 2, local_rows, hid)
    weights = lax.all_to_all(weights, both, split_axis=0, concat_axis=0, tiled=True)
    w_on = weights[:, 0].reshape(width, hid)
    w_tg = weights[:, 1].reshape(width, hid)
    full_next = lax.all_gather(next_feats, "tm", axis=1, tiled=True)
    full_obs = lax.all_gather(obs_feats, "tm", axis=1, tiled=True)

    all_step, keeping, all_reward, all_log_prob = small[0], small[1], small[2], small[3]
    rates = lax.dynamic_slice_in_dim(log_decay, mine * hid, hid)
    decay = jnp.exp(all_step[:, :, None] * rates)
    factor = decay * keeping[:, :, None]
    spread = jnp.sqrt(1.0 - decay * decay)
    later = lambda v: jnp.concatenate([v[:, 1:], jnp.zeros_like(v[:, :1])], axis=1)
    after = jnp.exp(later(all_step)[:, :, None] * rates) * later(keeping)[:, :, None]

    pad_heads = lambda v: jnp.pad(
        lax.dynamic_slice_in_dim(v, mine * hid, hid, axis=1) * scale_head,
        ((0, SUB - HEADS), (0, 0)),
    )
    heads_on, heads_tg = pad_heads(online_heads), pad_heads(target_heads)

    part_tg, _ = forward(full_next, w_tg, factor, spread, heads_tg, block)
    part_on, state_on = forward(full_obs, w_on, factor, spread, heads_on, block)
    q_all = lax.psum(
        jnp.concatenate([part_on[:, :HEADS], part_tg[:, :HEADS]], axis=1), "tm"
    )
    q_all = (
        q_all.reshape(count, 2 * HEADS, rows_b, block)
        .transpose(1, 2, 0, 3)
        .reshape(2 * HEADS, rows_b, length)
    )
    soft_value = jnp.minimum(q_all[HEADS], q_all[HEADS + 1]) - ENTROPY_COEFF * all_log_prob
    padded = lambda v: jnp.pad(v, ((0, 0), (0, NMAX)))
    returns = returns_from(
        padded(all_reward), padded(soft_value), padded(keeping), horizon, length
    )
    positions = jnp.arange(length, dtype=jnp.int32)
    weight_mask = (positions[None, :] >= burn_in[:, None]).astype(jnp.float32)
    slope = weight_mask * (q_all[:HEADS] - returns[None])
    dq = jnp.pad(
        slope.reshape(HEADS, rows_b, count, block)
        .transpose(2, 0, 1, 3)
        .reshape(count, HEADS, rows_b * block),
        ((0, 0), (0, SUB - HEADS), (0, 0)),
    )
    grad_u = backward(state_on, after, spread, dq, heads_on, block)
    term = (
        lax.dot_general(
            full_obs.reshape(rows_b * length, width),
            grad_u.reshape(rows_b * length, hid),
            (((0,), (0,)), ((), ())),
            preferred_element_type=jnp.float32,
        )
        * (width ** (-0.5))
    ).astype(jnp.bfloat16)
    terms = lax.all_to_all(term, both, split_axis=0, concat_axis=0, tiled=True)
    terms = terms.reshape(n_tm, n_b, local_rows, hid).astype(jnp.float32)
    grad_w = terms.sum(axis=1).transpose(1, 0, 2).reshape(local_rows, hidden)
    new_target = (1.0 - POLYAK_RATE) * target_w + POLYAK_RATE * (online_w - STEP_SIZE * grad_w)
    return (grad_w, new_target, lax.dynamic_slice_in_dim(returns, mine * span, span, axis=1))


def solution(mesh):
    return jax.shard_map(
        shards,
        mesh=mesh,
        in_specs=(
            P("batch", "tm", None),
            P("batch", "tm", None),
            P(("tm", "batch"), None),
            P(("tm", "batch"), None),
            P(),
            P("batch", "tm"),
            P(),
            P(),
            P("batch", "tm"),
            P("batch", "tm"),
            P("batch", "tm"),
            P("batch"),
            P("batch"),
        ),
        out_specs=(P(("tm", "batch"), None), P(("tm", "batch"), None), P("batch", "tm")),
        check_vma=False,
    )
```

```python
import functools

import jax
import jax.numpy as jnp
from jax import lax
from jax.experimental import pallas as pl
from jax.experimental.pallas import tpu as pltpu
from jax.sharding import PartitionSpec as P

NMAX = 8
SUB = 8
HEADS = 2

DISCOUNT = 0.99
ENTROPY_COEFF = 0.2
POLYAK_RATE = 0.005
STEP_SIZE = 0.1


def returns_from(ext_reward, ext_value, ext_keep, row_horizon, span):
    total = jnp.zeros((ext_reward.shape[0], span), jnp.float32)
    alive = jnp.ones((ext_reward.shape[0], span), jnp.float32)
    for offset in range(NMAX):
        inside = (row_horizon > offset)[:, None]
        total = total + jnp.where(
            inside, DISCOUNT**offset * alive * ext_reward[:, offset : offset + span], 0.0
        )
        alive = alive * ext_keep[:, offset + 1 : offset + 1 + span]
        finish = (row_horizon == offset + 1)[:, None]
        total = total + jnp.where(
            finish,
            DISCOUNT ** (offset + 1) * alive * ext_value[:, offset + 1 : offset + 1 + span],
            0.0,
        )
    return total


def tile_scan(gain, value, place, reverse):
    for shift in (1, 2, 4):
        if reverse:
            inside, move = place < SUB - shift, SUB - shift
        else:
            inside, move = place >= shift, shift
        other_gain = jnp.where(inside, pltpu.roll(gain, move, 1), 1.0)
        other_value = jnp.where(inside, pltpu.roll(value, move, 1), 0.0)
        value = value + gain * other_value
        gain = gain * other_gain
    return gain, value


def forward_kernel(
    input_scale, x_ref, w_ref, factor_ref, spread_ref, heads_ref, q_ref, state_ref, carry_ref
):
    rows_b, block, width = x_ref.shape
    hid = w_ref.shape[1]

    @pl.when(pl.program_id(0) == 0)
    def _():
        carry_ref[...] = jnp.zeros_like(carry_ref)

    proj = jnp.dot(
        x_ref[...].reshape(rows_b * block, width), w_ref[...], preferred_element_type=jnp.float32
    )
    drive = (proj * input_scale).reshape(rows_b, block, hid) * spread_ref[...]
    place = lax.broadcasted_iota(jnp.int32, (rows_b, SUB, hid), 1)
    carry = carry_ref[...]
    for tile in range(block // SUB):
        at = slice(tile * SUB, (tile + 1) * SUB)
        gain, value = tile_scan(factor_ref[:, at, :], drive[:, at, :], place, False)
        state = value + gain * carry
        state_ref[:, at, :] = state
        carry = jnp.broadcast_to(state[:, SUB - 1 : SUB, :], state.shape)
    carry_ref[...] = carry
    state = state_ref[...].reshape(rows_b * block, hid)
    act = state / (1.0 + jnp.exp(-state))
    q_ref[0] = lax.dot_general(
        heads_ref[...],
        act,
        (((1,), (1,)), ((), ())),
        precision=lax.Precision.HIGHEST,
        preferred_element_type=jnp.float32,
    )


def backward_kernel(state_ref, after_ref, spread_ref, dq_ref, heads_ref, du_ref, carry_ref):
    rows_b, block, hid = state_ref.shape

    @pl.when(pl.program_id(0) == 0)
    def _():
        carry_ref[...] = jnp.zeros_like(carry_ref)

    grad_y = lax.dot_general(
        dq_ref[0],
        heads_ref[...],
        (((0,), (0,)), ((), ())),
        precision=lax.Precision.HIGHEST,
        preferred_element_type=jnp.float32,
    ).reshape(rows_b, block, hid)
    state = state_ref[...]
    sigma = 1.0 / (1.0 + jnp.exp(-state))
    grad_h = grad_y * (sigma * (1.0 + state * (1.0 - sigma)))
    place = lax.broadcasted_iota(jnp.int32, (rows_b, SUB, hid), 1)
    carry = carry_ref[...]
    pieces = [None] * (block // SUB)
    for tile in reversed(range(block // SUB)):
        at = slice(tile * SUB, (tile + 1) * SUB)
        gain, value = tile_scan(after_ref[:, at, :], grad_h[:, at, :], place, True)
        adjoint = value + gain * carry
        pieces[tile] = spread_ref[:, at, :] * adjoint
        carry = jnp.broadcast_to(adjoint[:, 0:1, :], adjoint.shape)
    carry_ref[...] = carry
    du_ref[...] = jnp.concatenate(pieces, axis=1).astype(jnp.bfloat16)


def forward(x, w, factor, spread, heads, block):
    rows_b, length, width = x.shape
    hid = w.shape[1]
    count = length // block
    whole = lambda j: (0, 0)
    part = lambda j: (0, j, 0)
    return pl.pallas_call(
        functools.partial(forward_kernel, width ** (-0.5)),
        grid=(count,),
        in_specs=[
            pl.BlockSpec((rows_b, block, width), part),
            pl.BlockSpec((width, hid), whole),
            pl.BlockSpec((rows_b, block, hid), part),
            pl.BlockSpec((rows_b, block, hid), part),
            pl.BlockSpec(heads.shape, whole),
        ],
        out_specs=[
            pl.BlockSpec((1, heads.shape[0], rows_b * block), lambda j: (j, 0, 0)),
            pl.BlockSpec((rows_b, block, hid), part),
        ],
        out_shape=[
            jax.ShapeDtypeStruct((count, heads.shape[0], rows_b * block), jnp.float32),
            jax.ShapeDtypeStruct((rows_b, length, hid), jnp.float32),
        ],
        scratch_shapes=[pltpu.VMEM((rows_b, SUB, hid), jnp.float32)],
        compiler_params=pltpu.CompilerParams(dimension_semantics=("arbitrary",)),
        cost_estimate=pl.CostEstimate(
            flops=2 * rows_b * length * width * hid,
            bytes_accessed=x.size * 2 + w.size * 2 + 3 * factor.size * 4,
            transcendentals=2 * factor.size,
        ),
    )(x, w, factor, spread, heads)


def backward(state, after, spread, dq, heads, block):
    rows_b, length, hid = state.shape
    count = length // block
    part = lambda j: (0, count - 1 - j, 0)
    return pl.pallas_call(
        backward_kernel,
        grid=(count,),
        in_specs=[
            pl.BlockSpec((rows_b, block, hid), part),
            pl.BlockSpec((rows_b, block, hid), part),
            pl.BlockSpec((rows_b, block, hid), part),
            pl.BlockSpec((1, heads.shape[0], rows_b * block), lambda j: (count - 1 - j, 0, 0)),
            pl.BlockSpec(heads.shape, lambda j: (0, 0)),
        ],
        out_specs=pl.BlockSpec((rows_b, block, hid), part),
        out_shape=jax.ShapeDtypeStruct((rows_b, length, hid), jnp.bfloat16),
        scratch_shapes=[pltpu.VMEM((rows_b, SUB, hid), jnp.float32)],
        compiler_params=pltpu.CompilerParams(dimension_semantics=("arbitrary",)),
        cost_estimate=pl.CostEstimate(
            flops=40 * state.size,
            bytes_accessed=3 * state.size * 4 + state.size * 2,
            transcendentals=2 * state.size,
        ),
    )(state, after, spread, dq, heads)


def ring_place(index, count):
    if count & (count - 1):
        return index, lambda p: p
    place, shift = index, 1
    while shift < count:
        place = place ^ (index >> shift)
        shift += 1
    return place, lambda p: p ^ (p >> 1)


def greet(peers):
    barrier = pltpu.get_barrier_semaphore()
    for peer in peers:
        pl.semaphore_signal(
            barrier, inc=1, device_id={"tm": peer}, device_id_type=pl.DeviceIdType.MESH
        )
    pl.semaphore_wait(barrier, len(peers))


def gather_kernel(n, a_ref, b_ref, full_a, full_b, own_sem, out_sem, in_sem, pair_out, pair_in):
    pairs = n // 2
    me = lax.axis_index("tm")
    lane = lax.rem(me, 2)
    here, pair_at = ring_place(lax.div(me, 2), pairs)
    device_at = lambda step: pair_at(lax.rem(here + step + pairs, pairs)) * 2 + lane
    right, left, partner = device_at(1), device_at(-1), me + 1 - 2 * lane
    greet((right, left, partner) if pairs > 1 else (partner,))
    rows_b, span, _ = a_ref.shape

    def slot(full, owner, rows):
        return full.at[
            pl.ds(rows[0], rows[1]), pl.ds(pl.multiple_of(owner * span, span), span), :
        ]

    def send(src, dst, peer, out, arrived):
        copy = pltpu.make_async_remote_copy(
            src_ref=src,
            dst_ref=dst,
            send_sem=out,
            recv_sem=arrived,
            device_id={"tm": peer},
            device_id_type=pl.DeviceIdType.MESH,
        )
        copy.start()
        return copy

    whole, half = (0, rows_b), rows_b // 2
    hops = pairs // 2
    sources = ((a_ref, full_a), (b_ref, full_b))
    pending, pair_copies, ring = [], [], {}

    def rows_of(way, hop):
        if 2 * hop < pairs:
            return whole
        return (0, half) if way == 0 else (half, rows_b - half)

    def ring_send(which, way, hop):
        rows = rows_of(way, hop)
        if rows[1] == 0:
            return
        source, full = sources[which]
        back = -1 if way == 0 else 1
        owner = device_at(back * (hop - 1))
        src = source.at[pl.ds(rows[0], rows[1])] if hop == 1 else slot(full, owner, rows)
        ring[which, way, hop] = send(
            src,
            slot(full, owner, rows),
            right if way == 0 else left,
            out_sem.at[which, way, hop - 1],
            in_sem.at[which, way, hop - 1],
        )

    def pair_send(which, src, owner, rows, index):
        pair_copies.append(
            send(
                src,
                slot(sources[which][1], owner, rows),
                partner,
                pair_out.at[which, index],
                pair_in.at[which, index],
            )
        )

    for which in range(2):
        if hops:
            ring_send(which, 0, 1)
            ring_send(which, 1, 1)
    for which in range(2):
        source, full = sources[which]
        pair_send(which, source, me, whole, 0)
        own = pltpu.make_async_copy(source, slot(full, me, whole), own_sem.at[which])
        own.start()
        pending.append(own)
    for hop in range(1, hops + 1):
        for which in range(2):
            for way in range(2):
                if (which, way, hop) not in ring:
                    continue
                ring[which, way, hop].wait_recv()
                if hop < hops:
                    ring_send(which, way, hop + 1)
                rows = rows_of(way, hop)
                owner = device_at(-hop if way == 0 else hop)
                block = slot(sources[which][1], owner, rows)
                pair_send(which, block, owner, rows, 2 * hop - 1 + way)
    for copy in ring.values():
        copy.wait_send()
    for copy in pair_copies:
        copy.wait()
    for own in pending:
        own.wait()


def gather_two(a, b, n):
    rows_b, span, width = a.shape
    full = jax.ShapeDtypeStruct((rows_b, span * n, width), a.dtype)
    hops = max(n // 4, 1)
    return pl.pallas_call(
        functools.partial(gather_kernel, n),
        out_shape=[full, full],
        in_specs=[pl.BlockSpec(memory_space=pltpu.VMEM)] * 2,
        out_specs=[pl.BlockSpec(memory_space=pl.ANY)] * 2,
        scratch_shapes=[
            pltpu.SemaphoreType.DMA((2,)),
            pltpu.SemaphoreType.DMA((2, 2, hops)),
            pltpu.SemaphoreType.DMA((2, 2, hops)),
            pltpu.SemaphoreType.DMA((2, 2 * hops + 1)),
            pltpu.SemaphoreType.DMA((2, 2 * hops + 1)),
        ],
        compiler_params=pltpu.CompilerParams(collective_id=1, has_side_effects=True),
        cost_estimate=pl.CostEstimate(
            flops=0, bytes_accessed=96 * n * rows_b * span * width, transcendentals=0
        ),
    )(a, b)


def share_kernel(n, add, x_ref, o_ref, slots, send_sem, recv_sem):
    me = lax.axis_index("tm")
    peers = [lax.rem(me + step, n) for step in range(1, n)]
    greet(peers)
    copies = []
    for step, peer in enumerate(peers):
        copy = pltpu.make_async_remote_copy(
            src_ref=x_ref,
            dst_ref=slots.at[step] if add else o_ref.at[me],
            send_sem=send_sem.at[step],
            recv_sem=recv_sem.at[step],
            device_id={"tm": peer},
            device_id_type=pl.DeviceIdType.MESH,
        )
        copy.start()
        copies.append(copy)
    if not add:
        o_ref[me] = x_ref[...]
    for copy in copies:
        copy.wait()
    if add:
        total = x_ref[...]
        for step in range(n - 1):
            total = total + slots[step]
        o_ref[...] = total


def share(x, n, add, collective_id):
    shape = x.shape if add else (n,) + x.shape
    slots = (n - 1,) + x.shape if add else (SUB, 128)
    return pl.pallas_call(
        functools.partial(share_kernel, n, add),
        out_shape=jax.ShapeDtypeStruct(shape, x.dtype),
        in_specs=[pl.BlockSpec(memory_space=pltpu.VMEM)],
        out_specs=pl.BlockSpec(memory_space=pltpu.VMEM),
        scratch_shapes=[
            pltpu.VMEM(slots, x.dtype),
            pltpu.SemaphoreType.DMA((n - 1,)),
            pltpu.SemaphoreType.DMA((n - 1,)),
        ],
        compiler_params=pltpu.CompilerParams(
            collective_id=collective_id, has_side_effects=True
        ),
        cost_estimate=pl.CostEstimate(
            flops=x.size * n, bytes_accessed=x.size * 4 * n * 32, transcendentals=0
        ),
    )(x)


def shards(
    obs_feats,
    next_feats,
    online_w,
    target_w,
    log_decay,
    step_scale,
    online_heads,
    target_heads,
    reward,
    next_action_log_prob,
    resets,
    horizon,
    burn_in,
):
    rows_b, span, width = obs_feats.shape
    hidden = online_w.shape[1]
    n_tm, n_b = lax.axis_size("tm"), lax.axis_size("batch")
    length = span * n_tm
    hid = hidden // n_tm
    mine = lax.axis_index("tm")
    both = ("tm", "batch")
    block = span
    count = length // block
    scale_head = hidden ** (-0.5)
    local_rows = online_w.shape[0]

    small = jnp.stack([step_scale, 1.0 - resets.astype(jnp.float32), reward, next_action_log_prob])
    small = share(small.reshape(4 * rows_b, span), n_tm, False, 0)
    small = small.transpose(1, 0, 2).reshape(4, rows_b, length)
    weights = jnp.stack([online_w, target_w]).astype(jnp.bfloat16)
    weights = weights.reshape(2, local_rows, n_tm, hid).transpose(2, 0, 1, 3)
    weights = jnp.broadcast_to(
        weights[:, None], (n_tm, n_b, 2, local_rows, hid)
    ).reshape(n_tm * n_b, 2, local_rows, hid)
    weights = lax.all_to_all(weights, both, split_axis=0, concat_axis=0, tiled=True)
    w_on = weights[:, 0].reshape(width, hid)
    w_tg = weights[:, 1].reshape(width, hid)
    full_next, full_obs = gather_two(next_feats, obs_feats, n_tm)

    all_step, keeping, all_reward, all_log_prob = small[0], small[1], small[2], small[3]
    rates = lax.dynamic_slice_in_dim(log_decay, mine * hid, hid)
    decay = jnp.exp(all_step[:, :, None] * rates)
    factor = decay * keeping[:, :, None]
    spread = jnp.sqrt(1.0 - decay * decay)
    later = lambda v: jnp.concatenate([v[:, 1:], jnp.zeros_like(v[:, :1])], axis=1)
    after = jnp.exp(later(all_step)[:, :, None] * rates) * later(keeping)[:, :, None]

    pad_heads = lambda v: jnp.pad(
        lax.dynamic_slice_in_dim(v, mine * hid, hid, axis=1) * scale_head,
        ((0, SUB - HEADS), (0, 0)),
    )
    heads_on, heads_tg = pad_heads(online_heads), pad_heads(target_heads)

    part_tg, _ = forward(full_next, w_tg, factor, spread, heads_tg, block)
    part_on, state_on = forward(full_obs, w_on, factor, spread, heads_on, block)
    q_all = share(
        jnp.concatenate([part_on[:, :HEADS], part_tg[:, :HEADS]], axis=1), n_tm, True, 2
    )
    q_all = (
        q_all.reshape(count, 2 * HEADS, rows_b, block)
        .transpose(1, 2, 0, 3)
        .reshape(2 * HEADS, rows_b, length)
    )
    soft_value = jnp.minimum(q_all[HEADS], q_all[HEADS + 1]) - ENTROPY_COEFF * all_log_prob
    padded = lambda v: jnp.pad(v, ((0, 0), (0, NMAX)))
    returns = returns_from(
        padded(all_reward), padded(soft_value), padded(keeping), horizon, length
    )
    positions = jnp.arange(length, dtype=jnp.int32)
    weight_mask = (positions[None, :] >= burn_in[:, None]).astype(jnp.float32)
    slope = weight_mask * (q_all[:HEADS] - returns[None])
    dq = jnp.pad(
        slope.reshape(HEADS, rows_b, count, block)
        .transpose(2, 0, 1, 3)
        .reshape(count, HEADS, rows_b * block),
        ((0, 0), (0, SUB - HEADS), (0, 0)),
    )
    grad_u = backward(state_on, after, spread, dq, heads_on, block)
    term = (
        lax.dot_general(
            full_obs.reshape(rows_b * length, width),
            grad_u.reshape(rows_b * length, hid),
            (((0,), (0,)), ((), ())),
            preferred_element_type=jnp.float32,
        )
        * (width ** (-0.5))
    ).astype(jnp.bfloat16)
    terms = lax.all_to_all(term, both, split_axis=0, concat_axis=0, tiled=True)
    terms = terms.reshape(n_tm, n_b, local_rows, hid).astype(jnp.float32)
    grad_w = terms.sum(axis=1).transpose(1, 0, 2).reshape(local_rows, hidden)
    new_target = (1.0 - POLYAK_RATE) * target_w + POLYAK_RATE * (online_w - STEP_SIZE * grad_w)
    return (grad_w, new_target, lax.dynamic_slice_in_dim(returns, mine * span, span, axis=1))


def solution(mesh):
    return jax.shard_map(
        shards,
        mesh=mesh,
        in_specs=(
            P("batch", "tm", None),
            P("batch", "tm", None),
            P(("tm", "batch"), None),
            P(("tm", "batch"), None),
            P(),
            P("batch", "tm"),
            P(),
            P(),
            P("batch", "tm"),
            P("batch", "tm"),
            P("batch", "tm"),
            P("batch"),
            P("batch"),
        ),
        out_specs=(P(("tm", "batch"), None), P(("tm", "batch"), None), P("batch", "tm")),
        check_vma=False,
    )
```

```python
import functools

import jax
import jax.numpy as jnp
from jax import lax
from jax.experimental import pallas as pl
from jax.experimental.pallas import tpu as pltpu
from jax.sharding import PartitionSpec as P

NMAX = 8
SUB = 8
HEADS = 2

DISCOUNT = 0.99
ENTROPY_COEFF = 0.2
POLYAK_RATE = 0.005
STEP_SIZE = 0.1


def returns_from(ext_reward, ext_value, ext_keep, row_horizon, span):
    total = jnp.zeros((ext_reward.shape[0], span), jnp.float32)
    alive = jnp.ones((ext_reward.shape[0], span), jnp.float32)
    for offset in range(NMAX):
        inside = (row_horizon > offset)[:, None]
        total = total + jnp.where(
            inside, DISCOUNT**offset * alive * ext_reward[:, offset : offset + span], 0.0
        )
        alive = alive * ext_keep[:, offset + 1 : offset + 1 + span]
        finish = (row_horizon == offset + 1)[:, None]
        total = total + jnp.where(
            finish,
            DISCOUNT ** (offset + 1) * alive * ext_value[:, offset + 1 : offset + 1 + span],
            0.0,
        )
    return total


def tile_scan(gain, value, place, reverse):
    for shift in (1, 2, 4):
        if reverse:
            inside, move = place < SUB - shift, SUB - shift
        else:
            inside, move = place >= shift, shift
        other_gain = jnp.where(inside, pltpu.roll(gain, move, 1), 1.0)
        other_value = jnp.where(inside, pltpu.roll(value, move, 1), 0.0)
        value = value + gain * other_value
        gain = gain * other_gain
    return gain, value


def forward_kernel(
    input_scale, x_ref, w_ref, factor_ref, spread_ref, heads_ref, q_ref, state_ref, carry_ref
):
    rows_b, block, width = x_ref.shape
    hid = w_ref.shape[1]

    @pl.when(pl.program_id(0) == 0)
    def _():
        carry_ref[...] = jnp.zeros_like(carry_ref)

    proj = jnp.dot(
        x_ref[...].reshape(rows_b * block, width), w_ref[...], preferred_element_type=jnp.float32
    )
    drive = (proj * input_scale).reshape(rows_b, block, hid) * spread_ref[...]
    place = lax.broadcasted_iota(jnp.int32, (rows_b, SUB, hid), 1)
    carry = carry_ref[...]
    for tile in range(block // SUB):
        at = slice(tile * SUB, (tile + 1) * SUB)
        gain, value = tile_scan(factor_ref[:, at, :], drive[:, at, :], place, False)
        state = value + gain * carry
        state_ref[:, at, :] = state
        carry = jnp.broadcast_to(state[:, SUB - 1 : SUB, :], state.shape)
    carry_ref[...] = carry
    state = state_ref[...].reshape(rows_b * block, hid)
    act = state / (1.0 + jnp.exp(-state))
    q_ref[0] = lax.dot_general(
        heads_ref[...],
        act,
        (((1,), (1,)), ((), ())),
        precision=lax.Precision.HIGHEST,
        preferred_element_type=jnp.float32,
    )


def backward_kernel(state_ref, after_ref, spread_ref, dq_ref, heads_ref, du_ref, carry_ref):
    rows_b, block, hid = state_ref.shape

    @pl.when(pl.program_id(0) == 0)
    def _():
        carry_ref[...] = jnp.zeros_like(carry_ref)

    grad_y = lax.dot_general(
        dq_ref[0],
        heads_ref[...],
        (((0,), (0,)), ((), ())),
        precision=lax.Precision.HIGHEST,
        preferred_element_type=jnp.float32,
    ).reshape(rows_b, block, hid)
    state = state_ref[...]
    sigma = 1.0 / (1.0 + jnp.exp(-state))
    grad_h = grad_y * (sigma * (1.0 + state * (1.0 - sigma)))
    place = lax.broadcasted_iota(jnp.int32, (rows_b, SUB, hid), 1)
    carry = carry_ref[...]
    pieces = [None] * (block // SUB)
    for tile in reversed(range(block // SUB)):
        at = slice(tile * SUB, (tile + 1) * SUB)
        gain, value = tile_scan(after_ref[:, at, :], grad_h[:, at, :], place, True)
        adjoint = value + gain * carry
        pieces[tile] = spread_ref[:, at, :] * adjoint
        carry = jnp.broadcast_to(adjoint[:, 0:1, :], adjoint.shape)
    carry_ref[...] = carry
    du_ref[...] = jnp.concatenate(pieces, axis=1).astype(jnp.bfloat16)


def forward(x, w, factor, spread, heads, block):
    rows_b, length, width = x.shape
    hid = w.shape[1]
    count = length // block
    whole = lambda j: (0, 0)
    part = lambda j: (0, j, 0)
    return pl.pallas_call(
        functools.partial(forward_kernel, width ** (-0.5)),
        grid=(count,),
        in_specs=[
            pl.BlockSpec((rows_b, block, width), part),
            pl.BlockSpec((width, hid), whole),
            pl.BlockSpec((rows_b, block, hid), part),
            pl.BlockSpec((rows_b, block, hid), part),
            pl.BlockSpec(heads.shape, whole),
        ],
        out_specs=[
            pl.BlockSpec((1, heads.shape[0], rows_b * block), lambda j: (j, 0, 0)),
            pl.BlockSpec((rows_b, block, hid), part),
        ],
        out_shape=[
            jax.ShapeDtypeStruct((count, heads.shape[0], rows_b * block), jnp.float32),
            jax.ShapeDtypeStruct((rows_b, length, hid), jnp.float32),
        ],
        scratch_shapes=[pltpu.VMEM((rows_b, SUB, hid), jnp.float32)],
        compiler_params=pltpu.CompilerParams(dimension_semantics=("arbitrary",)),
        cost_estimate=pl.CostEstimate(
            flops=2 * rows_b * length * width * hid,
            bytes_accessed=x.size * 2 + w.size * 2 + 3 * factor.size * 4,
            transcendentals=2 * factor.size,
        ),
    )(x, w, factor, spread, heads)


def backward(state, after, spread, dq, heads, block):
    rows_b, length, hid = state.shape
    count = length // block
    part = lambda j: (0, count - 1 - j, 0)
    return pl.pallas_call(
        backward_kernel,
        grid=(count,),
        in_specs=[
            pl.BlockSpec((rows_b, block, hid), part),
            pl.BlockSpec((rows_b, block, hid), part),
            pl.BlockSpec((rows_b, block, hid), part),
            pl.BlockSpec((1, heads.shape[0], rows_b * block), lambda j: (count - 1 - j, 0, 0)),
            pl.BlockSpec(heads.shape, lambda j: (0, 0)),
        ],
        out_specs=pl.BlockSpec((rows_b, block, hid), part),
        out_shape=jax.ShapeDtypeStruct((rows_b, length, hid), jnp.bfloat16),
        scratch_shapes=[pltpu.VMEM((rows_b, SUB, hid), jnp.float32)],
        compiler_params=pltpu.CompilerParams(dimension_semantics=("arbitrary",)),
        cost_estimate=pl.CostEstimate(
            flops=40 * state.size,
            bytes_accessed=3 * state.size * 4 + state.size * 2,
            transcendentals=2 * state.size,
        ),
    )(state, after, spread, dq, heads)


def ring_place(index, count):
    if count & (count - 1):
        return index, lambda p: p
    place, shift = index, 1
    while shift < count:
        place = place ^ (index >> shift)
        shift += 1
    return place, lambda p: p ^ (p >> 1)


def greet(peers):
    barrier = pltpu.get_barrier_semaphore()
    for peer in peers:
        pl.semaphore_signal(
            barrier, inc=1, device_id={"tm": peer}, device_id_type=pl.DeviceIdType.MESH
        )
    pl.semaphore_wait(barrier, len(peers))


def gather_kernel(n, a_ref, b_ref, full_a, full_b, own_sem, out_sem, in_sem, pair_out, pair_in):
    pairs = n // 2
    me = lax.axis_index("tm")
    lane = lax.rem(me, 2)
    here, pair_at = ring_place(lax.div(me, 2), pairs)
    device_at = lambda step: pair_at(lax.rem(here + step + pairs, pairs)) * 2 + lane
    right, left, partner = device_at(1), device_at(-1), me + 1 - 2 * lane
    greet((right, left, partner) if pairs > 1 else (partner,))
    rows_b, span, _ = a_ref.shape

    def slot(full, owner, rows):
        return full.at[
            pl.ds(rows[0], rows[1]), pl.ds(pl.multiple_of(owner * span, span), span), :
        ]

    def send(src, dst, peer, out, arrived):
        copy = pltpu.make_async_remote_copy(
            src_ref=src,
            dst_ref=dst,
            send_sem=out,
            recv_sem=arrived,
            device_id={"tm": peer},
            device_id_type=pl.DeviceIdType.MESH,
        )
        copy.start()
        return copy

    whole, half = (0, rows_b), rows_b // 2
    hops = pairs // 2
    sources = ((a_ref, full_a), (b_ref, full_b))
    pending, pair_copies, ring = [], [], {}

    def rows_of(way, hop):
        if 2 * hop < pairs:
            return whole
        return (0, half) if way == 0 else (half, rows_b - half)

    def ring_send(which, way, hop):
        rows = rows_of(way, hop)
        if rows[1] == 0:
            return
        source, full = sources[which]
        back = -1 if way == 0 else 1
        owner = device_at(back * (hop - 1))
        src = source.at[pl.ds(rows[0], rows[1])] if hop == 1 else slot(full, owner, rows)
        ring[which, way, hop] = send(
            src,
            slot(full, owner, rows),
            right if way == 0 else left,
            out_sem.at[which, way, hop - 1],
            in_sem.at[which, way, hop - 1],
        )

    def pair_send(which, src, owner, rows, index):
        pair_copies.append(
            send(
                src,
                slot(sources[which][1], owner, rows),
                partner,
                pair_out.at[which, index],
                pair_in.at[which, index],
            )
        )

    for which in range(2):
        if hops:
            ring_send(which, 0, 1)
            ring_send(which, 1, 1)
    for which in range(2):
        source, full = sources[which]
        pair_send(which, source, me, whole, 0)
        own = pltpu.make_async_copy(source, slot(full, me, whole), own_sem.at[which])
        own.start()
        pending.append(own)
    for hop in range(1, hops + 1):
        for which in range(2):
            for way in range(2):
                if (which, way, hop) not in ring:
                    continue
                ring[which, way, hop].wait_recv()
                if hop < hops:
                    ring_send(which, way, hop + 1)
                rows = rows_of(way, hop)
                owner = device_at(-hop if way == 0 else hop)
                block = slot(sources[which][1], owner, rows)
                pair_send(which, block, owner, rows, 2 * hop - 1 + way)
    for copy in ring.values():
        copy.wait_send()
    for copy in pair_copies:
        copy.wait()
    for own in pending:
        own.wait()


def gather_two(a, b, n):
    rows_b, span, width = a.shape
    full = jax.ShapeDtypeStruct((rows_b, span * n, width), a.dtype)
    hops = max(n // 4, 1)
    return pl.pallas_call(
        functools.partial(gather_kernel, n),
        out_shape=[full, full],
        in_specs=[pl.BlockSpec(memory_space=pltpu.VMEM)] * 2,
        out_specs=[pl.BlockSpec(memory_space=pl.ANY)] * 2,
        scratch_shapes=[
            pltpu.SemaphoreType.DMA((2,)),
            pltpu.SemaphoreType.DMA((2, 2, hops)),
            pltpu.SemaphoreType.DMA((2, 2, hops)),
            pltpu.SemaphoreType.DMA((2, 2 * hops + 1)),
            pltpu.SemaphoreType.DMA((2, 2 * hops + 1)),
        ],
        compiler_params=pltpu.CompilerParams(collective_id=1, has_side_effects=True),
        cost_estimate=pl.CostEstimate(
            flops=0, bytes_accessed=96 * n * rows_b * span * width, transcendentals=0
        ),
    )(a, b)


def share_kernel(n, add, x_ref, o_ref, slots, send_sem, recv_sem):
    me = lax.axis_index("tm")
    peers = [lax.rem(me + step, n) for step in range(1, n)]
    greet(peers)
    copies = []
    for step, peer in enumerate(peers):
        copy = pltpu.make_async_remote_copy(
            src_ref=x_ref,
            dst_ref=slots.at[step] if add else o_ref.at[me],
            send_sem=send_sem.at[step],
            recv_sem=recv_sem.at[step],
            device_id={"tm": peer},
            device_id_type=pl.DeviceIdType.MESH,
        )
        copy.start()
        copies.append(copy)
    if not add:
        o_ref[me] = x_ref[...]
    for copy in copies:
        copy.wait()
    if add:
        total = x_ref[...]
        for step in range(n - 1):
            total = total + slots[step]
        o_ref[...] = total


def share(x, n, add, collective_id):
    shape = x.shape if add else (n,) + x.shape
    slots = (n - 1,) + x.shape if add else (SUB, 128)
    return pl.pallas_call(
        functools.partial(share_kernel, n, add),
        out_shape=jax.ShapeDtypeStruct(shape, x.dtype),
        in_specs=[pl.BlockSpec(memory_space=pltpu.VMEM)],
        out_specs=pl.BlockSpec(memory_space=pltpu.VMEM),
        scratch_shapes=[
            pltpu.VMEM(slots, x.dtype),
            pltpu.SemaphoreType.DMA((n - 1,)),
            pltpu.SemaphoreType.DMA((n - 1,)),
        ],
        compiler_params=pltpu.CompilerParams(
            collective_id=collective_id, has_side_effects=True
        ),
        cost_estimate=pl.CostEstimate(
            flops=x.size * n, bytes_accessed=x.size * 4 * n * 32, transcendentals=0
        ),
    )(x)


def shards(
    obs_feats,
    next_feats,
    online_w,
    target_w,
    log_decay,
    step_scale,
    online_heads,
    target_heads,
    reward,
    next_action_log_prob,
    resets,
    horizon,
    burn_in,
):
    rows_b, span, width = obs_feats.shape
    hidden = online_w.shape[1]
    n_tm, n_b = lax.axis_size("tm"), lax.axis_size("batch")
    length = span * n_tm
    hid = hidden // n_tm
    mine = lax.axis_index("tm")
    both = ("tm", "batch")
    block = span
    count = length // block
    scale_head = hidden ** (-0.5)
    local_rows = online_w.shape[0]

    small = jnp.stack([step_scale, 1.0 - resets.astype(jnp.float32), reward, next_action_log_prob])
    small = share(small.reshape(4 * rows_b, span), n_tm, False, 0)
    online_in, target_in, small = lax.optimization_barrier((online_w, target_w, small))
    small = small.transpose(1, 0, 2).reshape(4, rows_b, length)
    weights = jnp.stack([online_in, target_in]).astype(jnp.bfloat16)
    weights = weights.reshape(2, local_rows, n_tm, hid).transpose(2, 0, 1, 3)
    weights = jnp.broadcast_to(
        weights[:, None], (n_tm, n_b, 2, local_rows, hid)
    ).reshape(n_tm * n_b, 2, local_rows, hid)
    weights = lax.all_to_all(weights, both, split_axis=0, concat_axis=0, tiled=True)
    w_on = weights[:, 0].reshape(width, hid)
    w_tg = weights[:, 1].reshape(width, hid)
    full_next, full_obs = gather_two(next_feats, obs_feats, n_tm)

    all_step, keeping, all_reward, all_log_prob = small[0], small[1], small[2], small[3]
    rates = lax.dynamic_slice_in_dim(log_decay, mine * hid, hid)
    decay = jnp.exp(all_step[:, :, None] * rates)
    factor = decay * keeping[:, :, None]
    spread = jnp.sqrt(1.0 - decay * decay)
    later = lambda v: jnp.concatenate([v[:, 1:], jnp.zeros_like(v[:, :1])], axis=1)
    after = jnp.exp(later(all_step)[:, :, None] * rates) * later(keeping)[:, :, None]

    pad_heads = lambda v: jnp.pad(
        lax.dynamic_slice_in_dim(v, mine * hid, hid, axis=1) * scale_head,
        ((0, SUB - HEADS), (0, 0)),
    )
    heads_on, heads_tg = pad_heads(online_heads), pad_heads(target_heads)

    part_tg, _ = forward(full_next, w_tg, factor, spread, heads_tg, block)
    part_on, state_on = forward(full_obs, w_on, factor, spread, heads_on, block)
    q_all = share(
        jnp.concatenate([part_on[:, :HEADS], part_tg[:, :HEADS]], axis=1), n_tm, True, 2
    )
    q_all = (
        q_all.reshape(count, 2 * HEADS, rows_b, block)
        .transpose(1, 2, 0, 3)
        .reshape(2 * HEADS, rows_b, length)
    )
    soft_value = jnp.minimum(q_all[HEADS], q_all[HEADS + 1]) - ENTROPY_COEFF * all_log_prob
    padded = lambda v: jnp.pad(v, ((0, 0), (0, NMAX)))
    returns = returns_from(
        padded(all_reward), padded(soft_value), padded(keeping), horizon, length
    )
    positions = jnp.arange(length, dtype=jnp.int32)
    weight_mask = (positions[None, :] >= burn_in[:, None]).astype(jnp.float32)
    slope = weight_mask * (q_all[:HEADS] - returns[None])
    dq = jnp.pad(
        slope.reshape(HEADS, rows_b, count, block)
        .transpose(2, 0, 1, 3)
        .reshape(count, HEADS, rows_b * block),
        ((0, 0), (0, SUB - HEADS), (0, 0)),
    )
    grad_u = backward(state_on, after, spread, dq, heads_on, block)
    term = (
        lax.dot_general(
            full_obs.reshape(rows_b * length, width),
            grad_u.reshape(rows_b * length, hid),
            (((0,), (0,)), ((), ())),
            preferred_element_type=jnp.float32,
        )
        * (width ** (-0.5))
    ).astype(jnp.bfloat16)
    terms = lax.all_to_all(term, both, split_axis=0, concat_axis=0, tiled=True)
    terms = terms.reshape(n_tm, n_b, local_rows, hid).astype(jnp.float32)
    grad_w = terms.sum(axis=1).transpose(1, 0, 2).reshape(local_rows, hidden)
    new_target = (1.0 - POLYAK_RATE) * target_w + POLYAK_RATE * (online_w - STEP_SIZE * grad_w)
    return (grad_w, new_target, lax.dynamic_slice_in_dim(returns, mine * span, span, axis=1))


def solution(mesh):
    return jax.shard_map(
        shards,
        mesh=mesh,
        in_specs=(
            P("batch", "tm", None),
            P("batch", "tm", None),
            P(("tm", "batch"), None),
            P(("tm", "batch"), None),
            P(),
            P("batch", "tm"),
            P(),
            P(),
            P("batch", "tm"),
            P("batch", "tm"),
            P("batch", "tm"),
            P("batch"),
            P("batch"),
        ),
        out_specs=(P(("tm", "batch"), None), P(("tm", "batch"), None), P("batch", "tm")),
        check_vma=False,
    )
```
